32 devices in a mesh: ctx: 32 (over z, y, x, core).
Axes of the slice: x: 2, y: 2, z: 4, core: 2. Of those that a mesh axis runs over, the one named last changes fastest.
Arguments:
- queries: bfloat16 [8192, 768], P('ctx'), may hold values from -16 to 16
- keys: bfloat16 [8192, 768], P('ctx'), may hold values from -16 to 16
- values: bfloat16 [8192, 768], P('ctx'), may hold values from -6 to 6
- offsets: int32 [5, 12], replicated, may hold values from 0 to 31, as said below
Outputs:
- attended: bfloat16 [8192, 768], P('ctx')
The draws below stay inside these ranges and needn't reach their ends.
Inputs may be any that keep to these rules, and one draw needn't show every extreme that they name: offsets[l, h] lies in 0 to min(4 ** l, 32) - 1.
All inputs are finite; a program needn't handle non-finite values.
Results may differ from the reference program's by a relative error of at most 0.0035.
Values may be sent and summed in bfloat16 or wider, within the bound.
A program may use at most 64 MiB of HBM per device.

```python
import jax
import jax.numpy as jnp
from jax import lax

HEADS = 12
HEAD_DIM = 64
LEVELS = 5
TOK_DEV = 256
D = 768
SEQ = 8192
N_CTX = 32


def draw_keys(key, part):
    base = jax.random.normal(jax.random.fold_in(key, 11), (SEQ, D), jnp.float32)
    return jnp.clip(base, -16.0, 16.0).astype(jnp.bfloat16)


def draw_queries(key, part):
    base = jax.random.normal(jax.random.fold_in(key, 13), (SEQ, D), jnp.float32)
    return jnp.clip(base, -16.0, 16.0).astype(jnp.bfloat16)


def draw_offsets(key, part):
    spans = jnp.minimum(4 ** jnp.arange(LEVELS, dtype=jnp.int32), N_CTX)
    raw = jax.random.randint(jax.random.fold_in(key, 17), (LEVELS, HEADS), 0, 1 << 20)
    return (raw % spans[:, None]).astype(jnp.int32)


def levels(key, extent, split, smallest, top_value):
    def one(axis_at, shards_of):
        heights = jax.random.uniform(jax.random.fold_in(jax.random.fold_in(key, 6), axis_at), (shards_of,), jnp.float32, smallest / len(split), top_value / len(split))
        return jnp.repeat(jnp.exp(heights), extent[axis_at] // shards_of).reshape((-1,) + (1,) * (len(extent) - axis_at - 1))

    level = one(*split[0])
    for cut in split[1:]:
        level = level * one(*cut)
    return level


def scatter_about(stream_key, dims, spread, most, cuts=(), held_as=jnp.bfloat16):
    drawn = jax.random.normal(stream_key, dims, jnp.float32) * spread
    if len(cuts) > 0:
        drawn = levels(stream_key, dims, cuts, -0.22, 0.18) * drawn
    return jnp.clip(drawn, min=-most, max=most).astype(held_as)


def setup_inputs(seed: int = 0) -> dict:
    seeds = jax.random.split(jax.random.key(seed), 5)
    queries = draw_queries(jax.random.fold_in(seeds[4], 71), 0)
    keys = draw_keys(jax.random.fold_in(seeds[4], 71), 0)
    values = scatter_about(seeds[2], (SEQ, D), 1.0, 6.0, ((0, 32),))
    offsets = draw_offsets(jax.random.fold_in(seeds[4], 71), 0)
    return {"queries": queries, "keys": keys, "values": values, "offsets": offsets}


def attend_rows(query_rows, key_rows, value_rows, query_pos, key_pos, heads, scale):
    rows = query_rows.shape[0]
    cols = key_rows.shape[0]
    head_size = query_rows.shape[1] // heads
    query_heads = query_rows.reshape(rows, heads, head_size)
    key_heads = key_rows.reshape(cols, heads, head_size)
    value_heads = value_rows.reshape(cols, heads, head_size)
    allowed = key_pos[None, :] <= query_pos[:, None]
    scores = jnp.einsum("qhd,khd->hqk", query_heads, key_heads, preferred_element_type=jnp.float32) * scale
    scores = jnp.where(allowed[None], scores, -1e30)
    peak = jnp.max(scores, axis=2)
    weights = jnp.where(allowed[None], jnp.exp(scores - peak[:, :, None]), 0.0)
    totals = jnp.sum(weights, axis=2)
    result = jnp.einsum("hqk,khd->qhd", weights.astype(jnp.bfloat16), value_heads, preferred_element_type=jnp.float32)
    return result / totals.T[:, :, None], (peak + jnp.log(totals)).T


def causal_blocks(query_rows, key_rows, value_rows, heads, scale):
    length = query_rows.shape[0]
    block = min(512, length)
    outputs = []
    sums = []
    for number in range(length // block):
        query_pos = jnp.arange(number * block, (number + 1) * block, dtype=jnp.int32)
        key_pos = jnp.arange((number + 1) * block, dtype=jnp.int32)
        result, lse_part = attend_rows(query_rows[number * block:(number + 1) * block], key_rows[:(number + 1) * block], value_rows[:(number + 1) * block], query_pos, key_pos, heads, scale)
        outputs.append(result)
        sums.append(lse_part)
    return jnp.concatenate(outputs, 0), jnp.concatenate(sums, 0)


def select_rows(source, offset_row, group, heads):
    count = source.shape[0]
    head_size = source.shape[1] // heads
    shaped = source.reshape(count // group, group, heads, head_size)
    hit = jnp.arange(group, dtype=jnp.int32)[:, None] == offset_row.astype(jnp.int32)[None, :]
    picked = jnp.sum(jnp.where(hit[None, :, :, None], shaped, jnp.zeros((), source.dtype)), axis=1)
    return picked.astype(source.dtype).reshape(count // group, heads * head_size)


def merge_levels(base_out, base_lse, extras):
    rows_all, heads, head_size = base_out.shape
    best = base_lse
    numer = base_out
    denom = jnp.ones(base_lse.shape, jnp.float32)
    for level_out, level_lse, offset_row, group in extras:
        rows = level_out.shape[0]
        hit = jnp.arange(group, dtype=jnp.int32)[:, None] == offset_row.astype(jnp.int32)[None, :]
        best_g = best.reshape(rows, group, heads)
        lse_g = jnp.where(hit[None], level_lse[:, None], -1e30)
        newest = jnp.maximum(best_g, lse_g)
        keep_old = jnp.exp(best_g - newest)
        take_new = jnp.exp(lse_g - newest)
        numer = (numer.reshape(rows, group, heads, head_size) * keep_old[..., None] + level_out[:, None] * take_new[..., None]).reshape(rows_all, heads, head_size)
        denom = (denom.reshape(rows, group, heads) * keep_old + take_new).reshape(rows_all, heads)
        best = newest.reshape(rows_all, heads)
    merged = numer / denom[..., None]
    return merged.reshape(rows_all, -1).astype(jnp.bfloat16)


def reference(queries, keys, values, offsets):
    scale = HEAD_DIM ** -0.5
    level_outs = []
    level_lses = []
    for height in range(LEVELS):
        group = min(4 ** height, N_CTX)
        segments = SEQ // (TOK_DEV * group)
        picked_q = select_rows(queries, offsets[height], group, HEADS).reshape(segments, TOK_DEV, D)
        picked_k = select_rows(keys, offsets[height], group, HEADS).reshape(segments, TOK_DEV, D)
        picked_v = select_rows(values, offsets[height], group, HEADS).reshape(segments, TOK_DEV, D)
        outs, lses = lax.map(lambda triple: causal_blocks(triple[0], triple[1], triple[2], HEADS, scale), (picked_q, picked_k, picked_v))
        rows = TOK_DEV // group
        level_outs.append(outs.reshape(N_CTX, rows, HEADS, HEAD_DIM))
        level_lses.append(lses.reshape(N_CTX, rows, HEADS))

    def per_shard(shard_data):
        shard_outs, shard_lses = shard_data
        extras = []
        for height in range(1, LEVELS):
            extras.append((shard_outs[height], shard_lses[height], offsets[height], min(4 ** height, N_CTX)))
        return merge_levels(shard_outs[0], shard_lses[0], extras)

    shards = lax.map(per_shard, (tuple(level_outs), tuple(level_lses)))
    return shards.reshape(SEQ, D)
```

```python
import functools

import jax
import jax.numpy as jnp
from jax import lax
from jax.experimental import pallas as pl
from jax.experimental.pallas import tpu as pltpu
from jax.sharding import PartitionSpec as P

MESH = pl.DeviceIdType.MESH
NEG = -1e30
LAST = (((1,), (1,)), ((), ()))


def plan_of(levels, count, tokens, heads):
    plan = []
    late = False
    for height in range(1, levels):
        group = min(4**height, count)
        per = -(-heads // group)
        shift = 0
        if group >= 2 * heads:
            shift = group // 4 + (group // 2 - heads if late else 0)
            late = not late
        plan.append((height, group, tokens // group, per, shift))
    return plan


def is_packed(rows):
    return rows % 32 == 0


def up8(rows):
    return -(-rows // 8) * 8


def kind_of(rows):
    return jnp.bfloat16 if rows % 8 == 0 else jnp.float32


def halves(shape):
    return lax.broadcasted_iota(jnp.int32, shape, 1) < shape[1] // 2


def swap_halves(value):
    return pltpu.roll(value.astype(jnp.float32), value.shape[1] // 2, 1)


def attend(keys, queries, values_t):
    half = keys.shape[0] // 2
    scores = lax.dot_general(keys[:half], queries, LAST, preferred_element_type=jnp.float32)
    corner = lax.dot_general(
        keys[half:], queries[half:], LAST, preferred_element_type=jnp.float32
    )
    rows = lax.broadcasted_iota(jnp.int32, (half, half), 0)
    cols = lax.broadcasted_iota(jnp.int32, (half, half), 1)
    allowed = rows <= cols
    left = jnp.where(allowed, scores[:, :half], NEG)
    upper = scores[:, half:]
    lower = jnp.where(allowed, corner, NEG)
    peak_l = jnp.max(left, axis=0, keepdims=True)
    peak_r = jnp.maximum(
        jnp.max(upper, axis=0, keepdims=True), jnp.max(lower, axis=0, keepdims=True)
    )
    left = jnp.exp(left - peak_l).astype(jnp.bfloat16)
    upper = jnp.exp(upper - peak_r).astype(jnp.bfloat16)
    lower = jnp.exp(lower - peak_r).astype(jnp.bfloat16)
    out_l = jnp.dot(values_t[:, :half], left, preferred_element_type=jnp.float32)
    out_r = jnp.dot(
        values_t, jnp.concatenate([upper, lower], 0), preferred_element_type=jnp.float32
    )
    return jnp.concatenate([out_l, out_r], 1), jnp.concatenate([peak_l, peak_r], 1)


def places(plan, tokens):
    parts = []
    for _, group, rows, _, _ in plan:
        shape = (up8(rows), tokens)
        row = lax.broadcasted_iota(jnp.int32, shape, 0)
        col = lax.broadcasted_iota(jnp.int32, shape, 1)
        part = col - row * group
        parts.append(part if rows % 8 == 0 else jnp.where(row < rows, part, -1))
    return parts


def exchange_kernel(plan, heads, scale, offs_hbm, q_hbm, k_hbm, v_hbm, *refs):
    number = len(plan)
    base_out, base_peak, base_total, hits_out = refs[:4]
    back = refs[4 : 4 + number]
    refs = refs[4 + number :]
    offs, q_ref, k_ref, v_ref = refs[:4]
    refs = refs[4:]
    stage = refs[:number]
    inbox = refs[number : 2 * number]
    outbox = refs[2 * number : 3 * number]
    in_sem, send_sem, recv_sem, ret_send, ret_recv = refs[3 * number :]
    tokens, model = q_ref.shape
    size = model // heads
    pair = 2 * size
    pairs = heads // 2
    me = lax.axis_index("ctx")
    count = lax.axis_size("ctx")

    moves = [(offs_hbm, offs), (q_hbm, q_ref), (k_hbm, k_ref), (v_hbm, v_ref)]
    loads = [
        pltpu.make_async_copy(source, target, in_sem.at[i])
        for i, (source, target) in enumerate(moves)
    ]
    for load in loads:
        load.start()

    barrier = pltpu.get_barrier_semaphore()

    def greet(step, carry):
        other = lax.rem(me + step, count)
        pl.semaphore_signal(barrier, inc=1, device_id=(other,), device_id_type=MESH)
        return carry

    with jax.named_scope("greet"):
        lax.fori_loop(1, count, greet, 0)

    low = halves((tokens, pair))
    spans = [up8(entry[2]) for entry in plan]
    starts = [sum(spans[:at]) for at in range(number)]
    picked = sum(spans)
    low_p = halves((picked, pair))
    where_p = places(plan, tokens)

    with jax.named_scope("loadw"):
        for load in loads:
            load.wait()

    def pick(p, carry):
        cols = pl.ds(pl.multiple_of(p * pair, pair), pair)
        packed = jnp.concatenate([q_ref[:, cols], k_ref[:, cols], v_ref[:, cols]], 1)
        hits = []
        for side in range(2):
            for at, (height, *_) in enumerate(plan):
                hits.append(jnp.where(where_p[at] == offs[height, 2 * p + side], 1.0, 0.0))
        hit = jnp.concatenate(hits, 0).astype(jnp.bfloat16)
        hits_out[p] = hit
        both = jnp.dot(hit, packed, preferred_element_type=jnp.float32)
        for side in range(2):
            head = 2 * p + side
            got = both[side * picked : (side + 1) * picked]
            query, key, value = got[:, :pair], got[:, pair : 2 * pair], got[:, 2 * pair :]
            swapped = swap_halves(value)
            if side == 0:
                key = swap_halves(key)
            else:
                query = swap_halves(query)
                value, swapped = swapped, value
            left = jnp.where(low_p, query * scale, key)
            for at, (_, _, rows, _, _) in enumerate(plan):
                kind = stage[at].dtype
                first = starts[at]
                last = first + rows
                if is_packed(rows):
                    middle = first + rows // 2
                    right = jnp.where(
                        low_p[: rows // 2], value[first:middle], swapped[middle:last]
                    )
                    stage[at][head] = jnp.concatenate([left[first:last], right], 0).astype(kind)
                else:
                    stage[at][head] = jnp.concatenate(
                        [left[first:last], value[first:last]], 1
                    ).astype(kind)
        return carry

    with jax.named_scope("pick"):
        lax.fori_loop(0, pairs, pick, 0, unroll=3)
    with jax.named_scope("barw"):
        pl.semaphore_wait(barrier, count - 1)

    seats, seat = [], 0
    for _, _, _, per, _ in plan:
        seats.append(seat)
        seat += per

    def spot(at):
        _, group, _, _, shift = plan[at]
        mine = lax.rem(me, group)
        return mine, lax.rem(mine + group - shift, group)

    order = list(range(number))[::-1]
    with jax.named_scope("push"):
        for at in order:
            _, group, _, per, shift = plan[at]
            mine, _ = spot(at)
            for head in sorted(range(heads), key=lambda h: h % per):
                where = (shift + head // per) % group
                slot = head % per
                target = inbox[at].at[slot, mine]
                arrived = recv_sem.at[seats[at] + slot]

                @pl.when(mine != where)
                def _(at=at, head=head, where=where, target=target, arrived=arrived, mine=mine):
                    pltpu.make_async_remote_copy(
                        src_ref=stage[at].at[head],
                        dst_ref=target,
                        send_sem=send_sem.at[at],
                        recv_sem=arrived,
                        device_id=(me - mine + where,),
                        device_id_type=MESH,
                    ).start()

                @pl.when(mine == where)
                def _(at=at, head=head, target=target, arrived=arrived):
                    pltpu.make_async_copy(stage[at].at[head], target, arrived).start()

    ones = jnp.ones((16, tokens), jnp.bfloat16)
    row8 = lax.broadcasted_iota(jnp.int32, (8, tokens), 0)

    def base(p, carry):
        cols = pl.ds(pl.multiple_of(p * pair, pair), pair)
        query = q_ref[:, cols].astype(jnp.float32) * scale
        key = k_ref[:, cols]
        value_t = v_ref[:, cols].T
        for side in range(2):
            mask = low if side == 0 else jnp.logical_not(low)
            got, peak = attend(
                key,
                jnp.where(mask, query, 0.0).astype(jnp.bfloat16),
                jnp.concatenate([value_t[side * size : (side + 1) * size], ones], 0),
            )
            head = 2 * p + side
            base_out[head] = got[:size]
            base_peak[head] = jnp.where(row8 == number, peak, NEG)
            base_total[head] = jnp.where(row8 == number, got[size : size + 1], 1.0)
        return carry

    cuts = [pairs * part // 3 for part in range(4)]

    def bases(part):
        with jax.named_scope(f"base{part}"):
            lax.fori_loop(cuts[part], cuts[part + 1], base, 0, unroll=2)

    bases(0)

    def returning(at, slot, head, there):
        _, _, rows, _, _ = plan[at]
        mine, _ = spot(at)
        return pltpu.make_async_remote_copy(
            src_ref=outbox[at].at[slot, there],
            dst_ref=back[at].at[head, pl.ds(0, rows)],
            send_sem=ret_send.at[seats[at] + slot],
            recv_sem=ret_recv.at[at],
            device_id=(me - mine + there,),
            device_id_type=MESH,
        )

    row16 = lax.broadcasted_iota(jnp.int32, (16, tokens), 0)
    blank = jnp.zeros((pair - size - 16, tokens), jnp.bfloat16)

    for at in order:
        _, group, rows, per, _ = plan[at]
        if at == order[-1]:
            bases(1)
        for slot in range(per):
            mine, first_owner = spot(at)
            head = first_owner * per + slot

            @pl.when(head < heads)
            def _(at=at, group=group, rows=rows, slot=slot, head=head, mine=mine):
                with jax.named_scope(f"arr{at}_{slot}"):
                    pltpu.make_async_copy(
                        inbox[at].at[slot], inbox[at].at[slot], recv_sem.at[seats[at] + slot]
                    ).wait()
                block = inbox[at][slot]
                if is_packed(rows):
                    left = block[:, :rows].reshape(tokens, pair).astype(jnp.float32)
                    right = block[:, rows:].reshape(tokens // 2, pair).astype(jnp.float32)
                    split = (group, rows // 2, pair)
                    right = jnp.concatenate(
                        [right.reshape(split), swap_halves(right).reshape(split)], 1
                    ).reshape(tokens, pair)
                else:
                    block = block.reshape(tokens, 2 * pair)
                    left = block[:, :pair].astype(jnp.float32)
                    right = block[:, pair:].astype(jnp.float32)
                value = jnp.where(low, right, 1.0).astype(jnp.bfloat16)
                query = jnp.where(low, left, 0.0).astype(jnp.bfloat16)
                key = swap_halves(left).astype(jnp.bfloat16)
                value_t = value.T[: size + 16]
                got, peak = attend(key, query, value_t)
                sums = got[size : size + 1]
                lse = peak + jnp.log(sums)
                high = lse.astype(jnp.bfloat16).astype(jnp.float32)
                rest = lse - high
                mid = rest.astype(jnp.bfloat16).astype(jnp.float32)
                parts = jnp.where(row16 == 0, high, 0.0)
                parts = jnp.where(row16 == 1, mid, parts)
                parts = jnp.where(row16 == 2, rest - mid, parts)
                result = jnp.concatenate(
                    [
                        (got[:size] / sums).astype(jnp.bfloat16),
                        parts.astype(jnp.bfloat16),
                        blank,
                    ],
                    0,
                )
                outbox[at][slot] = (
                    result.T.reshape(group, rows, pair).astype(outbox[at].dtype)
                )

                def give(step, carry):
                    returning(at, slot, head, lax.rem(mine + step, group)).start()
                    return carry

                with jax.named_scope(f"give{at}_{slot}"):
                    pltpu.make_async_copy(
                        outbox[at].at[slot, mine],
                        back[at].at[head, pl.ds(0, rows)],
                        ret_recv.at[at],
                    ).start()
                    lax.fori_loop(1, group, give, 0, unroll=group <= 32)

    bases(2)

    for at in order:
        _, group, rows, per, _ = plan[at]
        _, first_owner = spot(at)
        owned = jnp.clip(heads - first_owner * per, 0, per)
        with jax.named_scope(f"coll{at}"):
            for many in range(per + 1):

                @pl.when(owned == many)
                def _(at=at, many=many):
                    sent = stage[at].at[pl.ds(0, heads - many)]
                    pltpu.make_async_copy(sent, sent, send_sem.at[at]).wait()

            landed = back[at].at[:, pl.ds(0, rows)]
            pltpu.make_async_copy(landed, landed, ret_recv.at[at]).wait()

    for at in order:
        _, group, _, per, _ = plan[at]
        _, first_owner = spot(at)
        for slot in range(per):

            @pl.when(first_owner * per + slot < heads)
            def _(at=at, group=group, slot=slot):
                gone = outbox[at].at[slot, pl.ds(0, group - 1)]
                pltpu.make_async_copy(gone, gone, ret_send.at[seats[at] + slot]).wait()


def merge_kernel(plan, heads, base_out, base_peak, base_total, hits, *refs):
    number = len(plan)
    back = refs[:number]
    out_hbm, out_vmem, sem = refs[number:]
    tokens, model = out_vmem.shape
    size = model // heads
    pair = 2 * size
    pairs = heads // 2
    spans = [up8(entry[2]) for entry in plan]
    picked = sum(spans)
    row8 = lax.broadcasted_iota(jnp.int32, (8, picked), 0)
    col8 = lax.broadcasted_iota(jnp.int32, (8, picked), 1)
    level = jnp.zeros((8, picked), jnp.int32)
    for at in range(1, number):
        level = jnp.where(col8 >= sum(spans[:at]), at, level)
    mine = row8 == level
    flag = jnp.where(mine, 1.0, 0.0)

    def leave(p):
        cols = pl.ds(p * pair, pair)
        return pltpu.make_async_copy(out_vmem.at[:, cols], out_hbm.at[:, cols], sem.at[p])

    for p in range(pairs):
        merged = []
        for side in range(2):
            head = 2 * p + side
            blocks = []
            for at, (_, _, rows, _, _) in enumerate(plan):
                block = back[at][head].astype(jnp.float32)
                if rows % 8:
                    kept = lax.broadcasted_iota(jnp.int32, block.shape, 0) < rows
                    block = jnp.where(kept, block, 0.0)
                blocks.append(block)
            sent_t = jnp.concatenate(blocks, 0).T
            parts = [
                jnp.where(mine, sent_t[size + i : size + i + 1], 0.0) for i in range(3)
            ]
            parts = jnp.concatenate(parts + [flag], 0).astype(jnp.bfloat16)
            hit = hits[p, side * picked : (side + 1) * picked]
            lses = jnp.dot(parts, hit, preferred_element_type=jnp.float32)
            lse = lses[:8] + lses[8:16] + lses[16:24]
            lse = jnp.where(lses[24:] > 0.5, lse, base_peak[head])
            best = jnp.max(lse, axis=0, keepdims=True)
            share = jnp.exp(lse - best)
            bottom = jnp.sum(share * base_total[head], axis=0, keepdims=True)
            share = share / bottom
            spread = jnp.concatenate(
                [
                    jnp.broadcast_to(share[at : at + 1], (spans[at], tokens))
                    for at in range(number)
                ],
                0,
            )
            moved = jnp.dot(
                sent_t[:size].astype(jnp.bfloat16),
                hit * spread.astype(jnp.bfloat16),
                preferred_element_type=jnp.float32,
            )
            merged.append(moved + share[number : number + 1] * base_out[head])
        both = jnp.concatenate(merged, 0).astype(jnp.bfloat16)
        out_vmem[:, pl.ds(p * pair, pair)] = both.T
        leave(p).start()
    for p in range(pairs):
        leave(p).wait()


def exchange_body(queries, keys, values, offsets):
    tokens, model = queries.shape
    levels, heads = offsets.shape
    count = lax.axis_size("ctx")
    plan = plan_of(levels, count, tokens, heads)
    size = model // heads
    pair = 2 * size
    number = len(plan)
    seats = sum(entry[3] for entry in plan)
    picked = sum(up8(entry[2]) for entry in plan)

    def block(rows):
        return (rows + rows // 2, pair) if is_packed(rows) else (rows, 2 * pair)

    scratch = [pltpu.SMEM((levels, heads), jnp.int32)]
    scratch += [pltpu.VMEM((tokens, model), jnp.bfloat16)] * 3
    for _, group, rows, per, _ in plan:
        scratch.append(pltpu.VMEM((heads, *block(rows)), kind_of(rows)))
    for _, group, rows, per, _ in plan:
        scratch.append(pltpu.VMEM((per, group, *block(rows)), kind_of(rows)))
    for _, group, rows, per, _ in plan:
        scratch.append(pltpu.VMEM((per, group, rows, pair), kind_of(rows)))
    scratch += [
        pltpu.SemaphoreType.DMA((4,)),
        pltpu.SemaphoreType.DMA((number,)),
        pltpu.SemaphoreType.DMA((seats,)),
        pltpu.SemaphoreType.DMA((seats,)),
        pltpu.SemaphoreType.DMA((number,)),
    ]
    outs = [
        pltpu.VMEM((heads, size, tokens), jnp.float32),
        pltpu.VMEM((heads, 8, tokens), jnp.float32),
        pltpu.VMEM((heads, 8, tokens), jnp.float32),
        pltpu.VMEM((heads // 2, 2 * picked, tokens), jnp.bfloat16),
    ]
    for _, _, rows, _, _ in plan:
        outs.append(pltpu.VMEM((heads, up8(rows), pair), kind_of(rows)))
    scale = size**-0.5
    vmem = pl.BlockSpec(memory_space=pltpu.VMEM)
    far = pl.BlockSpec(memory_space=pl.ANY)
    parts = pl.pallas_call(
        functools.partial(exchange_kernel, plan, heads, scale),
        out_shape=outs,
        in_specs=[far, far, far, far],
        out_specs=[vmem] * len(outs),
        scratch_shapes=scratch,
        compiler_params=pltpu.CompilerParams(collective_id=0, has_side_effects=True),
    )(offsets, queries, keys, values)
    return pl.pallas_call(
        functools.partial(merge_kernel, plan, heads),
        out_shape=jax.ShapeDtypeStruct((tokens, model), jnp.bfloat16),
        in_specs=[vmem] * len(outs),
        out_specs=far,
        scratch_shapes=[
            pltpu.VMEM((tokens, model), jnp.bfloat16),
            pltpu.SemaphoreType.DMA((heads // 2,)),
        ],
        compiler_params=pltpu.CompilerParams(vmem_limit_bytes=16 * 1024 * 1024),
    )(*parts)


def solution(mesh):
    in_specs = (P("ctx", None), P("ctx", None), P("ctx", None), P())
    out_specs = P("ctx", None)
    return jax.shard_map(
        exchange_body, mesh=mesh, in_specs=in_specs, out_specs=out_specs, check_vma=False
    )
```

```python
import functools

import jax
import jax.numpy as jnp
from jax import lax
from jax.experimental import pallas as pl
from jax.experimental.pallas import tpu as pltpu
from jax.sharding import PartitionSpec as P

MESH = pl.DeviceIdType.MESH
NEG = -1e30
LAST = (((1,), (1,)), ((), ()))


def plan_of(levels, count, tokens, heads):
    plan = []
    late = False
    for height in range(1, levels):
        group = min(4**height, count)
        per = -(-heads // group)
        shift = 0
        if group >= 2 * heads:
            shift = (group // 4 + (1 if late else -1) * (group // 2 - heads)) % group
            late = not late
        plan.append((height, group, tokens // group, per, shift))
    return plan


def is_packed(rows):
    return rows % 16 == 0


def is_folded(rows):
    return rows % 32 == 0


def returned(rows):
    return rows // 2 + 8 if is_folded(rows) else rows


def held(rows):
    return rows // 2 + 8 if is_folded(rows) else up8(rows)


def up8(rows):
    return -(-rows // 8) * 8


def kind_of(rows):
    return jnp.bfloat16 if rows % 8 == 0 else jnp.float32


def halves(shape):
    return lax.broadcasted_iota(jnp.int32, shape, 1) < shape[1] // 2


def swap_halves(value):
    return pltpu.roll(value.astype(jnp.float32), value.shape[1] // 2, 1)


def attend(keys, queries, values_t):
    half = keys.shape[0] // 2
    scores = lax.dot_general(keys[:half], queries, LAST, preferred_element_type=jnp.float32)
    corner = lax.dot_general(
        keys[half:], queries[half:], LAST, preferred_element_type=jnp.float32
    )
    rows = lax.broadcasted_iota(jnp.int32, (half, half), 0)
    cols = lax.broadcasted_iota(jnp.int32, (half, half), 1)
    allowed = rows <= cols
    left = jnp.where(allowed, scores[:, :half], NEG)
    upper = scores[:, half:]
    lower = jnp.where(allowed, corner, NEG)
    peak_l = jnp.max(left, axis=0, keepdims=True)
    peak_r = jnp.maximum(
        jnp.max(upper, axis=0, keepdims=True), jnp.max(lower, axis=0, keepdims=True)
    )
    left = jnp.exp(left - peak_l).astype(jnp.bfloat16)
    upper = jnp.exp(upper - peak_r).astype(jnp.bfloat16)
    lower = jnp.exp(lower - peak_r).astype(jnp.bfloat16)
    out_l = jnp.dot(values_t[:, :half], left, preferred_element_type=jnp.float32)
    out_r = jnp.dot(
        values_t, jnp.concatenate([upper, lower], 0), preferred_element_type=jnp.float32
    )
    return jnp.concatenate([out_l, out_r], 1), jnp.concatenate([peak_l, peak_r], 1)


def places(plan, tokens):
    parts = []
    for _, group, rows, _, _ in plan:
        shape = (up8(rows), tokens)
        row = lax.broadcasted_iota(jnp.int32, shape, 0)
        col = lax.broadcasted_iota(jnp.int32, shape, 1)
        part = col - row * group
        parts.append(part if rows % 8 == 0 else jnp.where(row < rows, part, -1))
    return parts


def exchange_kernel(plan, heads, scale, offs_hbm, q_hbm, k_hbm, v_hbm, *refs):
    number = len(plan)
    base_out, base_peak, base_total, hits_out = refs[:4]
    back = refs[4 : 4 + number]
    refs = refs[4 + number :]
    offs, q_ref, k_ref, v_ref = refs[:4]
    refs = refs[4:]
    stage = refs[:number]
    inbox = refs[number : 2 * number]
    outbox = refs[2 * number : 3 * number]
    in_sem, send_sem, recv_sem, ret_send, ret_recv = refs[3 * number :]
    tokens, model = q_ref.shape
    size = model // heads
    pair = 2 * size
    pairs = heads // 2
    me = lax.axis_index("ctx")
    count = lax.axis_size("ctx")

    moves = [(offs_hbm, offs), (q_hbm, q_ref), (k_hbm, k_ref), (v_hbm, v_ref)]
    loads = [
        pltpu.make_async_copy(source, target, in_sem.at[i])
        for i, (source, target) in enumerate(moves)
    ]
    for load in loads:
        load.start()

    barrier = pltpu.get_barrier_semaphore()

    def greet(step, carry):
        other = lax.rem(me + step, count)
        pl.semaphore_signal(barrier, inc=1, device_id=(other,), device_id_type=MESH)
        return carry

    with jax.named_scope("greet"):
        lax.fori_loop(1, count, greet, 0)

    low = halves((tokens, pair))
    spans = [up8(entry[2]) for entry in plan]
    starts = [sum(spans[:at]) for at in range(number)]
    picked = sum(spans)
    low_p = halves((picked, pair))
    where_p = places(plan, tokens)

    with jax.named_scope("loadw"):
        for load in loads:
            load.wait()

    def pick(p, carry):
        cols = pl.ds(pl.multiple_of(p * pair, pair), pair)
        packed = jnp.concatenate([q_ref[:, cols], k_ref[:, cols], v_ref[:, cols]], 1)
        hits = []
        for side in range(2):
            for at, (height, *_) in enumerate(plan):
                hits.append(jnp.where(where_p[at] == offs[height, 2 * p + side], 1.0, 0.0))
        hit = jnp.concatenate(hits, 0).astype(jnp.bfloat16)
        hits_out[p] = hit
        both = jnp.dot(hit, packed, preferred_element_type=jnp.float32)
        for side in range(2):
            head = 2 * p + side
            got = both[side * picked : (side + 1) * picked]
            query, key, value = got[:, :pair], got[:, pair : 2 * pair], got[:, 2 * pair :]
            swapped = swap_halves(value)
            if side == 0:
                key = swap_halves(key)
            else:
                query = swap_halves(query)
                value, swapped = swapped, value
            left = jnp.where(low_p, query * scale, key)
            for at, (_, _, rows, _, _) in enumerate(plan):
                kind = stage[at].dtype
                first = starts[at]
                last = first + rows
                if is_packed(rows):
                    middle = first + rows // 2
                    right = jnp.where(
                        low_p[: rows // 2], value[first:middle], swapped[middle:last]
                    )
                    stage[at][head] = jnp.concatenate([left[first:last], right], 0).astype(kind)
                else:
                    stage[at][head] = jnp.concatenate(
                        [left[first:last], value[first:last]], 1
                    ).astype(kind)
        return carry

    with jax.named_scope("pick"):
        lax.fori_loop(0, pairs, pick, 0, unroll=3)
    with jax.named_scope("barw"):
        pl.semaphore_wait(barrier, count - 1)

    seats, seat = [], 0
    for _, _, _, per, _ in plan:
        seats.append(seat)
        seat += per

    def spot(at):
        _, group, _, _, shift = plan[at]
        mine = lax.rem(me, group)
        return mine, lax.rem(mine + group - shift, group)

    order = list(range(number))[::-1]

    def push(at):
        _, group, _, per, shift = plan[at]
        mine, _ = spot(at)
        for head in sorted(range(heads), key=lambda h: h % per):
            where = (shift + head // per) % group
            slot = head % per
            target = inbox[at].at[slot, mine]
            arrived = recv_sem.at[seats[at] + slot]

            @pl.when(mine != where)
            def _(head=head, where=where, target=target, arrived=arrived):
                pltpu.make_async_remote_copy(
                    src_ref=stage[at].at[head],
                    dst_ref=target,
                    send_sem=send_sem.at[at],
                    recv_sem=arrived,
                    device_id=(me - mine + where,),
                    device_id_type=MESH,
                ).start()

            @pl.when(mine == where)
            def _(head=head, target=target, arrived=arrived):
                pltpu.make_async_copy(stage[at].at[head], target, arrived).start()

    ones = jnp.ones((16, tokens), jnp.bfloat16)
    row8 = lax.broadcasted_iota(jnp.int32, (8, tokens), 0)

    def base(p, carry):
        cols = pl.ds(pl.multiple_of(p * pair, pair), pair)
        query = q_ref[:, cols].astype(jnp.float32) * scale
        key = k_ref[:, cols]
        value_t = v_ref[:, cols].T
        for side in range(2):
            mask = low if side == 0 else jnp.logical_not(low)
            got, peak = attend(
                key,
                jnp.where(mask, query, 0.0).astype(jnp.bfloat16),
                jnp.concatenate([value_t[side * size : (side + 1) * size], ones], 0),
            )
            head = 2 * p + side
            base_out[head] = got[:size]
            base_peak[head] = jnp.where(row8 == number, peak, NEG)
            base_total[head] = jnp.where(row8 == number, got[size : size + 1], 1.0)
        return carry

    def bases(start, stop):
        start, stop = pairs * start // 6, pairs * stop // 6
        with jax.named_scope(f"base{start}"):
            lax.fori_loop(start, stop, base, 0, unroll=2)


    def returning(at, slot, head, there):
        _, _, rows, _, _ = plan[at]
        mine, _ = spot(at)
        return pltpu.make_async_remote_copy(
            src_ref=outbox[at].at[slot, there],
            dst_ref=back[at].at[head, pl.ds(0, rows)],
            send_sem=ret_send.at[seats[at] + slot],
            recv_sem=ret_recv.at[at],
            device_id=(me - mine + there,),
            device_id_type=MESH,
        )

    row16 = lax.broadcasted_iota(jnp.int32, (16, tokens), 0)
    blank = jnp.zeros((pair - size - 16, tokens), jnp.bfloat16)

    def serve(at, slot):
        _, group, rows, per, _ = plan[at]
        mine, first_owner = spot(at)
        head = first_owner * per + slot

        @pl.when(head < heads)
        def _():
            with jax.named_scope(f"arr{at}_{slot}"):
                pltpu.make_async_copy(
                    inbox[at].at[slot], inbox[at].at[slot], recv_sem.at[seats[at] + slot]
                ).wait()
            block = inbox[at][slot]
            if is_packed(rows):
                left = block[:, :rows].reshape(tokens, pair).astype(jnp.float32)
                right = block[:, rows:].reshape(tokens // 2, pair).astype(jnp.float32)
                split = (group, rows // 2, pair)
                right = jnp.concatenate(
                    [right.reshape(split), swap_halves(right).reshape(split)], 1
                ).reshape(tokens, pair)
            else:
                block = block.reshape(tokens, 2 * pair)
                left = block[:, :pair].astype(jnp.float32)
                right = block[:, pair:].astype(jnp.float32)
            value = jnp.where(low, right, 1.0).astype(jnp.bfloat16)
            query = jnp.where(low, left, 0.0).astype(jnp.bfloat16)
            key = swap_halves(left).astype(jnp.bfloat16)
            value_t = value.T[: size + 16]
            got, peak = attend(key, query, value_t)
            sums = got[size : size + 1]
            lse = peak + jnp.log(sums)
            high = lse.astype(jnp.bfloat16).astype(jnp.float32)
            rest = lse - high
            mid = rest.astype(jnp.bfloat16).astype(jnp.float32)
            parts = jnp.where(row16 == 0, high, 0.0)
            parts = jnp.where(row16 == 1, mid, parts)
            parts = jnp.where(row16 == 2, rest - mid, parts)
            result = jnp.concatenate(
                [
                    (got[:size] / sums).astype(jnp.bfloat16),
                    parts.astype(jnp.bfloat16),
                    blank,
                ],
                0,
            )
            outbox[at][slot] = (
                result.T.reshape(group, rows, pair).astype(outbox[at].dtype)
            )

            def give(step, carry):
                returning(at, slot, head, lax.rem(mine + step, group)).start()
                return carry

            with jax.named_scope(f"give{at}_{slot}"):
                pltpu.make_async_copy(
                    outbox[at].at[slot, mine],
                    back[at].at[head, pl.ds(0, rows)],
                    ret_recv.at[at],
                ).start()
                lax.fori_loop(1, group, give, 0, unroll=group <= 32)

    for at in order[:-1]:
        with jax.named_scope(f"push{at}"):
            push(at)
    bases(0, 2)
    with jax.named_scope("push0"):
        push(0)
    bases(2, 4)
    for at in order[:-1]:
        for slot in range(plan[at][3]):
            serve(at, slot)
    for slot in range(plan[0][3]):
        serve(0, slot)
    bases(4, 6)
    for at in order:
        _, group, rows, per, _ = plan[at]
        _, first_owner = spot(at)
        owned = jnp.clip(heads - first_owner * per, 0, per)
        with jax.named_scope(f"coll{at}"):
            for many in range(per + 1):

                @pl.when(owned == many)
                def _(at=at, many=many):
                    sent = stage[at].at[pl.ds(0, heads - many)]
                    pltpu.make_async_copy(sent, sent, send_sem.at[at]).wait()

            landed = back[at].at[:, pl.ds(0, rows)]
            pltpu.make_async_copy(landed, landed, ret_recv.at[at]).wait()

    for at in order:
        _, group, _, per, _ = plan[at]
        _, first_owner = spot(at)
        for slot in range(per):

            @pl.when(first_owner * per + slot < heads)
            def _(at=at, group=group, slot=slot):
                gone = outbox[at].at[slot, pl.ds(0, group - 1)]
                pltpu.make_async_copy(gone, gone, ret_send.at[seats[at] + slot]).wait()


def merge_kernel(plan, heads, base_out, base_peak, base_total, hits, *refs):
    number = len(plan)
    back = refs[:number]
    out_hbm, out_vmem, sem = refs[number:]
    tokens, model = out_vmem.shape
    size = model // heads
    pair = 2 * size
    pairs = heads // 2
    spans = [up8(entry[2]) for entry in plan]
    picked = sum(spans)
    row8 = lax.broadcasted_iota(jnp.int32, (8, picked), 0)
    col8 = lax.broadcasted_iota(jnp.int32, (8, picked), 1)
    level = jnp.zeros((8, picked), jnp.int32)
    for at in range(1, number):
        level = jnp.where(col8 >= sum(spans[:at]), at, level)
    mine = row8 == level
    flag = jnp.where(mine, 1.0, 0.0)

    def leave(p):
        cols = pl.ds(p * pair, pair)
        return pltpu.make_async_copy(out_vmem.at[:, cols], out_hbm.at[:, cols], sem.at[p])

    sents, sums, shares = {}, {}, {}
    for p in range(pairs):
        for side in range(2):
            head = 2 * p + side
            blocks = []
            for at, (_, _, rows, _, _) in enumerate(plan):
                block = back[at][head].astype(jnp.float32)
                if rows % 8:
                    kept = lax.broadcasted_iota(jnp.int32, block.shape, 0) < rows
                    block = jnp.where(kept, block, 0.0)
                blocks.append(block)
            sent_t = jnp.concatenate(blocks, 0).astype(jnp.bfloat16).T
            hit = hits[p, side * picked : (side + 1) * picked]
            tails = sent_t[size : size + 16].astype(jnp.float32)
            parts = [jnp.where(mine, tails[i : i + 1], 0.0) for i in range(3)]
            parts = jnp.concatenate(parts + [flag], 0).astype(jnp.bfloat16)
            lses = jnp.dot(parts, hit, preferred_element_type=jnp.float32)
            sents[head], sums[head] = sent_t, lses
    for p in range(pairs):
        for side in range(2):
            head = 2 * p + side
            lses = sums[head]
            lse = lses[:8] + lses[8:16] + lses[16:24]
            lse = jnp.where(lses[24:] > 0.5, lse, base_peak[head])
            best = jnp.max(lse, axis=0, keepdims=True)
            share = jnp.exp(lse - best)
            bottom = jnp.sum(share * base_total[head], axis=0, keepdims=True)
            share = share / bottom
            shares[head] = share
    for p in range(pairs):
        merged = []
        for side in range(2):
            head = 2 * p + side
            sent_t, share = sents[head], shares[head]
            hit = hits[p, side * picked : (side + 1) * picked]
            spread = jnp.concatenate(
                [
                    jnp.broadcast_to(share[at : at + 1], (spans[at], tokens))
                    for at in range(number)
                ],
                0,
            )
            moved = jnp.dot(
                sent_t[:size],
                hit * spread.astype(jnp.bfloat16),
                preferred_element_type=jnp.float32,
            )
            merged.append(moved + share[number : number + 1] * base_out[head])
        both = jnp.concatenate(merged, 0).astype(jnp.bfloat16)
        out_vmem[:, pl.ds(p * pair, pair)] = both.T
        leave(p).start()
    for p in range(pairs):
        leave(p).wait()


def exchange_body(queries, keys, values, offsets):
    tokens, model = queries.shape
    levels, heads = offsets.shape
    count = lax.axis_size("ctx")
    plan = plan_of(levels, count, tokens, heads)
    size = model // heads
    pair = 2 * size
    number = len(plan)
    seats = sum(entry[3] for entry in plan)
    picked = sum(up8(entry[2]) for entry in plan)

    def block(rows):
        return (rows + rows // 2, pair) if is_packed(rows) else (rows, 2 * pair)

    scratch = [pltpu.SMEM((levels, heads), jnp.int32)]
    scratch += [pltpu.VMEM((tokens, model), jnp.bfloat16)] * 3
    for _, group, rows, per, _ in plan:
        scratch.append(pltpu.VMEM((heads, *block(rows)), kind_of(rows)))
    for _, group, rows, per, _ in plan:
        scratch.append(pltpu.VMEM((per, group, *block(rows)), kind_of(rows)))
    for _, group, rows, per, _ in plan:
        scratch.append(pltpu.VMEM((per, group, rows, pair), kind_of(rows)))
    scratch += [
        pltpu.SemaphoreType.DMA((4,)),
        pltpu.SemaphoreType.DMA((number,)),
        pltpu.SemaphoreType.DMA((seats,)),
        pltpu.SemaphoreType.DMA((seats,)),
        pltpu.SemaphoreType.DMA((number,)),
    ]
    outs = [
        pltpu.VMEM((heads, size, tokens), jnp.float32),
        pltpu.VMEM((heads, 8, tokens), jnp.float32),
        pltpu.VMEM((heads, 8, tokens), jnp.float32),
        pltpu.VMEM((heads // 2, 2 * picked, tokens), jnp.bfloat16),
    ]
    for _, _, rows, _, _ in plan:
        outs.append(pltpu.VMEM((heads, up8(rows), pair), kind_of(rows)))
    scale = size**-0.5
    vmem = pl.BlockSpec(memory_space=pltpu.VMEM)
    far = pl.BlockSpec(memory_space=pl.ANY)
    parts = pl.pallas_call(
        functools.partial(exchange_kernel, plan, heads, scale),
        out_shape=outs,
        in_specs=[far, far, far, far],
        out_specs=[vmem] * len(outs),
        scratch_shapes=scratch,
        compiler_params=pltpu.CompilerParams(collective_id=0, has_side_effects=True),
    )(offsets, queries, keys, values)
    return pl.pallas_call(
        functools.partial(merge_kernel, plan, heads),
        out_shape=jax.ShapeDtypeStruct((tokens, model), jnp.bfloat16),
        in_specs=[vmem] * len(outs),
        out_specs=far,
        scratch_shapes=[
            pltpu.VMEM((tokens, model), jnp.bfloat16),
            pltpu.SemaphoreType.DMA((heads // 2,)),
        ],
        compiler_params=pltpu.CompilerParams(vmem_limit_bytes=16 * 1024 * 1024),
    )(*parts)


def solution(mesh):
    in_specs = (P("ctx", None), P("ctx", None), P("ctx", None), P())
    out_specs = P("ctx", None)
    return jax.shard_map(
        exchange_body, mesh=mesh, in_specs=in_specs, out_specs=out_specs, check_vma=False
    )
```

```python
import functools

import jax
import jax.numpy as jnp
from jax import lax
from jax.experimental import pallas as pl
from jax.experimental.pallas import tpu as pltpu
from jax.sharding import PartitionSpec as P

MESH = pl.DeviceIdType.MESH
NEG = -1e30
LINE = 4
LAST = (((1,), (1,)), ((), ()))


def plan_of(levels, count, tokens, heads):
    plan = []
    wide = 0
    for height in range(1, levels):
        group = min(4**height, count)
        per = -(-heads // group)
        first, step = 0, 1
        if group >= 2 * heads:
            first, step = wide % 2, 2
            wide += 1
        elif group > heads:
            first = group - heads
        owners = [first + step * (head // per) for head in range(heads)]
        plan.append((height, group, tokens // group, per, owners))
    return plan


def is_packed(rows):
    return rows % 16 == 0


def up8(rows):
    return -(-rows // 8) * 8


def kind_of(rows):
    return jnp.bfloat16 if rows % 8 == 0 else jnp.float32


def halves(shape):
    return lax.broadcasted_iota(jnp.int32, shape, 1) < shape[1] // 2


def swap_halves(value):
    return pltpu.roll(value.astype(jnp.float32), value.shape[1] // 2, 1)


def attend(keys, queries, values_t):
    half = keys.shape[0] // 2
    scores = lax.dot_general(keys[:half], queries, LAST, preferred_element_type=jnp.float32)
    corner = lax.dot_general(
        keys[half:], queries[half:], LAST, preferred_element_type=jnp.float32
    )
    rows = lax.broadcasted_iota(jnp.int32, (half, half), 0)
    cols = lax.broadcasted_iota(jnp.int32, (half, half), 1)
    allowed = rows <= cols
    left = jnp.where(allowed, scores[:, :half], NEG)
    upper = scores[:, half:]
    lower = jnp.where(allowed, corner, NEG)
    peak_l = jnp.max(left, axis=0, keepdims=True)
    peak_r = jnp.maximum(
        jnp.max(upper, axis=0, keepdims=True), jnp.max(lower, axis=0, keepdims=True)
    )
    left = jnp.exp(left - peak_l).astype(jnp.bfloat16)
    upper = jnp.exp(upper - peak_r).astype(jnp.bfloat16)
    lower = jnp.exp(lower - peak_r).astype(jnp.bfloat16)
    out_l = jnp.dot(values_t[:, :half], left, preferred_element_type=jnp.float32)
    out_r = jnp.dot(
        values_t, jnp.concatenate([upper, lower], 0), preferred_element_type=jnp.float32
    )
    return jnp.concatenate([out_l, out_r], 1), jnp.concatenate([peak_l, peak_r], 1)


def places(plan, tokens):
    parts = []
    for _, group, rows, _, _ in plan:
        shape = (up8(rows), tokens)
        row = lax.broadcasted_iota(jnp.int32, shape, 0)
        col = lax.broadcasted_iota(jnp.int32, shape, 1)
        part = col - row * group
        parts.append(part if rows % 8 == 0 else jnp.where(row < rows, part, -1))
    return parts


def exchange_kernel(plan, heads, scale, offs_hbm, q_hbm, k_hbm, v_hbm, *refs):
    number = len(plan)
    base_out, base_peak, base_total, hits_out = refs[:4]
    back = refs[4 : 4 + number]
    refs = refs[4 + number :]
    offs, q_ref, k_ref, v_ref = refs[:4]
    refs = refs[4:]
    stage = refs[:number]
    inbox = refs[number : 2 * number]
    outbox = refs[2 * number : 3 * number]
    in_sem, send_sem, recv_sem, ret_send, ret_recv, high_sem = refs[3 * number :]
    tokens, model = q_ref.shape
    size = model // heads
    pair = 2 * size
    pairs = heads // 2
    me = lax.axis_index("ctx")
    count = lax.axis_size("ctx")

    moves = [(offs_hbm, offs), (q_hbm, q_ref), (k_hbm, k_ref), (v_hbm, v_ref)]
    loads = [
        pltpu.make_async_copy(source, target, in_sem.at[i])
        for i, (source, target) in enumerate(moves)
    ]
    for load in loads:
        load.start()

    barrier = pltpu.get_barrier_semaphore()
    block = count // LINE
    line = lax.div(me, block)
    seat_in = me - line * block

    def tell(sem, other):
        pl.semaphore_signal(sem, inc=1, device_id=(other,), device_id_type=MESH)

    def greet(step, carry):
        tell(barrier, line * block + lax.rem(seat_in + step, block))
        return carry

    def greet_above(step, carry):
        tell(barrier, line * block + block + step)
        return carry

    with jax.named_scope("greet"):
        lax.fori_loop(1, block, greet, 0)
        lax.fori_loop(0, (LINE - 1 - line) * block, greet_above, 0)

    def hear(first, last):
        for at in range(LINE):
            for above in range(max(first, at + 1), last + 1):

                @pl.when(line == at)
                def _(above=above):
                    pl.semaphore_wait(high_sem.at[above], 1)

    low = halves((tokens, pair))
    spans = [up8(entry[2]) for entry in plan]
    starts = [sum(spans[:at]) for at in range(number)]
    picked = sum(spans)
    low_p = halves((picked, pair))
    where_p = places(plan, tokens)

    def meet():
        with jax.named_scope("barw"):
            pl.semaphore_wait(barrier, block - 1 + line * block)

        for at in range(1, LINE):
            for below in range(at):

                @pl.when(line == at)
                def _(at=at, below=below):
                    tell(high_sem.at[at], me - (at - below) * block)

    soon = line < LINE // 2

    @pl.when(jnp.logical_not(soon))
    def _():
        meet()

    with jax.named_scope("loadw"):
        for load in loads:
            load.wait()

    def pick(p, carry):
        cols = pl.ds(pl.multiple_of(p * pair, pair), pair)
        packed = jnp.concatenate([q_ref[:, cols], k_ref[:, cols], v_ref[:, cols]], 1)
        hits = []
        for side in range(2):
            for at, (height, *_) in enumerate(plan):
                hits.append(jnp.where(where_p[at] == offs[height, 2 * p + side], 1.0, 0.0))
        hit = jnp.concatenate(hits, 0).astype(jnp.bfloat16)
        hits_out[p] = hit
        both = jnp.dot(hit, packed, preferred_element_type=jnp.float32)
        for side in range(2):
            head = 2 * p + side
            got = both[side * picked : (side + 1) * picked]
            query, key, value = got[:, :pair], got[:, pair : 2 * pair], got[:, 2 * pair :]
            swapped = swap_halves(value)
            if side == 0:
                key = swap_halves(key)
            else:
                query = swap_halves(query)
                value, swapped = swapped, value
            left = jnp.where(low_p, query * scale, key)
            for at, (_, _, rows, *_) in enumerate(plan):
                kind = stage[at].dtype
                first = starts[at]
                last = first + rows
                if is_packed(rows):
                    middle = first + rows // 2
                    right = jnp.where(
                        low_p[: rows // 2], value[first:middle], swapped[middle:last]
                    )
                    stage[at][head] = jnp.concatenate([left[first:last], right], 0).astype(kind)
                else:
                    stage[at][head] = jnp.concatenate(
                        [left[first:last], value[first:last]], 1
                    ).astype(kind)
        return carry

    with jax.named_scope("pick"):
        lax.fori_loop(0, pairs, pick, 0, unroll=3)
    @pl.when(soon)
    def _():
        meet()

    seats, seat = [], 0
    for _, _, _, per, *_ in plan:
        seats.append(seat)
        seat += per

    def spot(at):
        _, group, _, per, owners = plan[at]
        mine = lax.rem(me, group)
        found = heads
        for head in range(0, heads, per):
            found = jnp.where(mine == owners[head], head, found)
        return mine, found

    spots = [spot(at) for at in range(number)]
    order = list(range(number))[::-1]

    def push(at, slots=None, only=None):
        _, group, _, per, *_ = plan[at]
        mine, _ = spots[at]
        for head in sorted(range(heads), key=lambda h: h % per):
            where = plan[at][4][head]
            slot = head % per
            if only is not None and head != only:
                continue
            if slots is not None and slot not in slots:
                continue
            target = inbox[at].at[slot, mine]
            arrived = recv_sem.at[seats[at] + slot]

            @pl.when(mine != where)
            def _(head=head, where=where, target=target, arrived=arrived):
                pltpu.make_async_remote_copy(
                    src_ref=stage[at].at[head],
                    dst_ref=target,
                    send_sem=send_sem.at[at],
                    recv_sem=arrived,
                    device_id=(me - mine + where,),
                    device_id_type=MESH,
                ).start()

            @pl.when(mine == where)
            def _(head=head, target=target, arrived=arrived):
                pltpu.make_async_copy(stage[at].at[head], target, arrived).start()

    ones = jnp.ones((16, tokens), jnp.bfloat16)
    row8 = lax.broadcasted_iota(jnp.int32, (8, tokens), 0)

    def base(p, carry):
        cols = pl.ds(pl.multiple_of(p * pair, pair), pair)
        query = q_ref[:, cols].astype(jnp.float32) * scale
        key = k_ref[:, cols]
        value_t = v_ref[:, cols].T
        for side in range(2):
            mask = low if side == 0 else jnp.logical_not(low)
            got, peak = attend(
                key,
                jnp.where(mask, query, 0.0).astype(jnp.bfloat16),
                jnp.concatenate([value_t[side * size : (side + 1) * size], ones], 0),
            )
            head = 2 * p + side
            base_out[head] = got[:size]
            base_peak[head] = jnp.where(row8 == number, peak, NEG)
            base_total[head] = jnp.where(row8 == number, got[size : size + 1], 1.0)
        return carry

    def bases(start, stop):
        start, stop = pairs * start // 6, pairs * stop // 6
        with jax.named_scope(f"base{start}"):
            lax.fori_loop(start, stop, base, 0, unroll=2)


    def returning(at, slot, head, there):
        _, _, rows, *_ = plan[at]
        mine, _ = spots[at]
        return pltpu.make_async_remote_copy(
            src_ref=outbox[at].at[slot, there],
            dst_ref=back[at].at[head, pl.ds(0, rows)],
            send_sem=ret_send.at[seats[at] + slot],
            recv_sem=ret_recv.at[at],
            device_id=(me - mine + there,),
            device_id_type=MESH,
        )

    row16 = lax.broadcasted_iota(jnp.int32, (16, tokens), 0)
    blank = jnp.zeros((pair - size - 16, tokens), jnp.bfloat16)

    def serve(at, slot):
        _, group, rows, per, *_ = plan[at]
        mine, first = spots[at]
        head = first + slot

        @pl.when(head < heads)
        def _():
            with jax.named_scope(f"arr{at}_{slot}"):
                pltpu.make_async_copy(
                    inbox[at].at[slot], inbox[at].at[slot], recv_sem.at[seats[at] + slot]
                ).wait()
            block = inbox[at][slot]
            if is_packed(rows):
                left = block[:, :rows].reshape(tokens, pair).astype(jnp.float32)
                right = block[:, rows:].reshape(tokens // 2, pair).astype(jnp.float32)
                split = (group, rows // 2, pair)
                right = jnp.concatenate(
                    [right.reshape(split), swap_halves(right).reshape(split)], 1
                ).reshape(tokens, pair)
            else:
                block = block.reshape(tokens, 2 * pair)
                left = block[:, :pair].astype(jnp.float32)
                right = block[:, pair:].astype(jnp.float32)
            value = jnp.where(low, right, 1.0).astype(jnp.bfloat16)
            query = jnp.where(low, left, 0.0).astype(jnp.bfloat16)
            key = swap_halves(left).astype(jnp.bfloat16)
            value_t = value.T[: size + 16]
            got, peak = attend(key, query, value_t)
            sums = got[size : size + 1]
            lse = peak + jnp.log(sums)
            high = lse.astype(jnp.bfloat16).astype(jnp.float32)
            rest = lse - high
            mid = rest.astype(jnp.bfloat16).astype(jnp.float32)
            parts = jnp.where(row16 == 0, high, 0.0)
            parts = jnp.where(row16 == 1, mid, parts)
            parts = jnp.where(row16 == 2, rest - mid, parts)
            result = jnp.concatenate(
                [
                    (got[:size] / sums).astype(jnp.bfloat16),
                    parts.astype(jnp.bfloat16),
                    blank,
                ],
                0,
            )
            outbox[at][slot] = (
                result.T.reshape(group, rows, pair).astype(outbox[at].dtype)
            )

            def give(step, carry):
                returning(at, slot, head, lax.rem(mine + step, group)).start()
                return carry

            with jax.named_scope(f"give{at}_{slot}"):
                pltpu.make_async_copy(
                    outbox[at].at[slot, mine],
                    back[at].at[head, pl.ds(0, rows)],
                    ret_recv.at[at],
                ).start()
                lax.fori_loop(1, group, give, 0, unroll=group <= 32)

    last = line == LINE - 1
    soon_slots = range(1)
    rest_slots = range(1, plan[0][3])

    @pl.when(jnp.logical_not(last))
    def _():
        with jax.named_scope("push0"):
            push(0, soon_slots)

    @pl.when(soon)
    def _():
        bases(0, 2)

    far = [at for at in order if plan[at][1] >= 2 * heads]
    close = [at for at in order[:-1] if at not in far]

    @pl.when(soon)
    def _():
        hear(1, 1)
        for at in close:
            push(at)

    with jax.named_scope("hear"):
        hear(2, LINE - 2)
    with jax.named_scope("push1"):
        for head in range(heads):
            for at in far:
                push(at, only=head)

    @pl.when(jnp.logical_not(soon))
    def _():
        hear(LINE - 1, LINE - 1)
        for at in close:
            push(at)

    @pl.when(last)
    def _():
        with jax.named_scope("push0b"):
            push(0)

    @pl.when(jnp.logical_not(last))
    def _():
        with jax.named_scope("push0c"):
            push(0, rest_slots)

    with jax.named_scope("late"):
        pl.when(soon)(lambda: hear(LINE - 1, LINE - 1))

    @pl.when(jnp.logical_not(soon))
    def _():
        bases(0, 2)

    wide = [(at, slot) for at in order[:-1] for slot in range(plan[at][3])]
    tall = [(0, slot) for slot in range(plan[0][3])]

    def serve_all(jobs):
        for at, slot in jobs:
            serve(at, slot)

    @pl.when(last)
    def _():
        serve_all(wide + tall)

    @pl.when(soon)
    def _():
        serve_all(tall[:1] + wide[-1:] + wide[:-1] + tall[1:])

    @pl.when(jnp.logical_not(jnp.logical_or(soon, last)))
    def _():
        serve_all(tall[:1] + wide + tall[1:])

    bases(2, 6)
    for at in order:
        _, group, rows, per, *_ = plan[at]
        _, first = spots[at]
        owned = jnp.clip(heads - first, 0, per)
        with jax.named_scope(f"coll{at}"):
            for many in range(per + 1):

                @pl.when(owned == many)
                def _(at=at, many=many):
                    sent = stage[at].at[pl.ds(0, heads - many)]
                    pltpu.make_async_copy(sent, sent, send_sem.at[at]).wait()

            landed = back[at].at[:, pl.ds(0, rows)]
            pltpu.make_async_copy(landed, landed, ret_recv.at[at]).wait()

    for at in order:
        _, group, _, per, *_ = plan[at]
        _, first = spots[at]
        for slot in range(per):

            @pl.when(first + slot < heads)
            def _(at=at, group=group, slot=slot):
                gone = outbox[at].at[slot, pl.ds(0, group - 1)]
                pltpu.make_async_copy(gone, gone, ret_send.at[seats[at] + slot]).wait()


def merge_kernel(plan, heads, base_out, base_peak, base_total, hits, *refs):
    number = len(plan)
    back = refs[:number]
    out_hbm, out_vmem, sem = refs[number:]
    tokens, model = out_vmem.shape
    size = model // heads
    pair = 2 * size
    pairs = heads // 2
    spans = [up8(entry[2]) for entry in plan]
    picked = sum(spans)
    row8 = lax.broadcasted_iota(jnp.int32, (8, picked), 0)
    col8 = lax.broadcasted_iota(jnp.int32, (8, picked), 1)
    level = jnp.zeros((8, picked), jnp.int32)
    for at in range(1, number):
        level = jnp.where(col8 >= sum(spans[:at]), at, level)
    mine = row8 == level
    flag = jnp.where(mine, 1.0, 0.0)

    def leave(p):
        cols = pl.ds(p * pair, pair)
        return pltpu.make_async_copy(out_vmem.at[:, cols], out_hbm.at[:, cols], sem.at[p])

    sents, sums, shares = {}, {}, {}
    for p in range(pairs):
        for side in range(2):
            head = 2 * p + side
            blocks = []
            for at, (_, _, rows, *_) in enumerate(plan):
                block = back[at][head].astype(jnp.float32)
                if rows % 8:
                    kept = lax.broadcasted_iota(jnp.int32, block.shape, 0) < rows
                    block = jnp.where(kept, block, 0.0)
                blocks.append(block)
            sent_t = jnp.concatenate(blocks, 0).astype(jnp.bfloat16).T
            hit = hits[p, side * picked : (side + 1) * picked]
            tails = sent_t[size : size + 16].astype(jnp.float32)
            parts = [jnp.where(mine, tails[i : i + 1], 0.0) for i in range(3)]
            parts = jnp.concatenate(parts + [flag], 0).astype(jnp.bfloat16)
            lses = jnp.dot(parts, hit, preferred_element_type=jnp.float32)
            sents[head], sums[head] = sent_t, lses
    for p in range(pairs):
        for side in range(2):
            head = 2 * p + side
            lses = sums[head]
            lse = lses[:8] + lses[8:16] + lses[16:24]
            lse = jnp.where(lses[24:] > 0.5, lse, base_peak[head])
            best = jnp.max(lse, axis=0, keepdims=True)
            share = jnp.exp(lse - best)
            bottom = jnp.sum(share * base_total[head], axis=0, keepdims=True)
            share = share / bottom
            shares[head] = share
    for p in range(pairs):
        merged = []
        for side in range(2):
            head = 2 * p + side
            sent_t, share = sents[head], shares[head]
            hit = hits[p, side * picked : (side + 1) * picked]
            spread = jnp.concatenate(
                [
                    jnp.broadcast_to(share[at : at + 1], (spans[at], tokens))
                    for at in range(number)
                ],
                0,
            )
            moved = jnp.dot(
                sent_t[:size],
                hit * spread.astype(jnp.bfloat16),
                preferred_element_type=jnp.float32,
            )
            merged.append(moved + share[number : number + 1] * base_out[head])
        both = jnp.concatenate(merged, 0).astype(jnp.bfloat16)
        out_vmem[:, pl.ds(p * pair, pair)] = both.T
        leave(p).start()
    for p in range(pairs):
        leave(p).wait()


def exchange_body(queries, keys, values, offsets):
    tokens, model = queries.shape
    levels, heads = offsets.shape
    count = lax.axis_size("ctx")
    plan = plan_of(levels, count, tokens, heads)
    size = model // heads
    pair = 2 * size
    number = len(plan)
    seats = sum(entry[3] for entry in plan)
    picked = sum(up8(entry[2]) for entry in plan)

    def block(rows):
        return (rows + rows // 2, pair) if is_packed(rows) else (rows, 2 * pair)

    scratch = [pltpu.SMEM((levels, heads), jnp.int32)]
    scratch += [pltpu.VMEM((tokens, model), jnp.bfloat16)] * 3
    for _, group, rows, per, *_ in plan:
        scratch.append(pltpu.VMEM((heads, *block(rows)), kind_of(rows)))
    for _, group, rows, per, *_ in plan:
        scratch.append(pltpu.VMEM((per, group, *block(rows)), kind_of(rows)))
    for _, group, rows, per, *_ in plan:
        scratch.append(pltpu.VMEM((per, group, rows, pair), kind_of(rows)))
    scratch += [
        pltpu.SemaphoreType.DMA((4,)),
        pltpu.SemaphoreType.DMA((number,)),
        pltpu.SemaphoreType.DMA((seats,)),
        pltpu.SemaphoreType.DMA((seats,)),
        pltpu.SemaphoreType.DMA((number,)),
        pltpu.SemaphoreType.REGULAR((LINE,)),
    ]
    outs = [
        pltpu.VMEM((heads, size, tokens), jnp.float32),
        pltpu.VMEM((heads, 8, tokens), jnp.float32),
        pltpu.VMEM((heads, 8, tokens), jnp.float32),
        pltpu.VMEM((heads // 2, 2 * picked, tokens), jnp.bfloat16),
    ]
    for _, _, rows, *_ in plan:
        outs.append(pltpu.VMEM((heads, up8(rows), pair), kind_of(rows)))
    scale = size**-0.5
    vmem = pl.BlockSpec(memory_space=pltpu.VMEM)
    far = pl.BlockSpec(memory_space=pl.ANY)
    parts = pl.pallas_call(
        functools.partial(exchange_kernel, plan, heads, scale),
        out_shape=outs,
        in_specs=[far, far, far, far],
        out_specs=[vmem] * len(outs),
        scratch_shapes=scratch,
        compiler_params=pltpu.CompilerParams(collective_id=0, has_side_effects=True),
    )(offsets, queries, keys, values)
    return pl.pallas_call(
        functools.partial(merge_kernel, plan, heads),
        out_shape=jax.ShapeDtypeStruct((tokens, model), jnp.bfloat16),
        in_specs=[vmem] * len(outs),
        out_specs=far,
        scratch_shapes=[
            pltpu.VMEM((tokens, model), jnp.bfloat16),
            pltpu.SemaphoreType.DMA((heads // 2,)),
        ],
        compiler_params=pltpu.CompilerParams(vmem_limit_bytes=16 * 1024 * 1024),
    )(*parts)


def solution(mesh):
    in_specs = (P("ctx", None), P("ctx", None), P("ctx", None), P())
    out_specs = P("ctx", None)
    return jax.shard_map(
        exchange_body, mesh=mesh, in_specs=in_specs, out_specs=out_specs, check_vma=False
    )
```

```python
import functools

import jax
import jax.numpy as jnp
from jax import lax
from jax.experimental import pallas as pl
from jax.experimental.pallas import tpu as pltpu
from jax.sharding import PartitionSpec as P

MESH = pl.DeviceIdType.MESH
NEG = -1e30
LINE = 4
LAST = (((1,), (1,)), ((), ()))


def plan_of(levels, count, tokens, heads):
    plan = []
    wide = 0
    for height in range(1, levels):
        group = min(4**height, count)
        per = -(-heads // group)
        first, step = 0, 1
        if group >= 2 * heads:
            first, step = wide % 2, 2
            wide += 1
        elif group > heads:
            first = group - heads
        owners = [first + step * (head // per) for head in range(heads)]
        plan.append((height, group, tokens // group, per, owners))
    return plan


def is_packed(rows):
    return rows % 16 == 0


def up8(rows):
    return -(-rows // 8) * 8


def kind_of(rows):
    return jnp.bfloat16 if rows % 8 == 0 else jnp.float32


def halves(shape):
    return lax.broadcasted_iota(jnp.int32, shape, 1) < shape[1] // 2


def swap_halves(value):
    return pltpu.roll(value.astype(jnp.float32), value.shape[1] // 2, 1)


def attend(keys, queries, values_t):
    half = keys.shape[0] // 2
    scores = lax.dot_general(keys[:half], queries, LAST, preferred_element_type=jnp.float32)
    corner = lax.dot_general(
        keys[half:], queries[half:], LAST, preferred_element_type=jnp.float32
    )
    rows = lax.broadcasted_iota(jnp.int32, (half, half), 0)
    cols = lax.broadcasted_iota(jnp.int32, (half, half), 1)
    allowed = rows <= cols
    left = jnp.where(allowed, scores[:, :half], NEG)
    upper = scores[:, half:]
    lower = jnp.where(allowed, corner, NEG)
    peak_l = jnp.max(left, axis=0, keepdims=True)
    peak_r = jnp.maximum(
        jnp.max(upper, axis=0, keepdims=True), jnp.max(lower, axis=0, keepdims=True)
    )
    left = jnp.exp(left - peak_l).astype(jnp.bfloat16)
    upper = jnp.exp(upper - peak_r).astype(jnp.bfloat16)
    lower = jnp.exp(lower - peak_r).astype(jnp.bfloat16)
    out_l = jnp.dot(values_t[:, :half], left, preferred_element_type=jnp.float32)
    out_r = jnp.dot(
        values_t, jnp.concatenate([upper, lower], 0), preferred_element_type=jnp.float32
    )
    return jnp.concatenate([out_l, out_r], 1), jnp.concatenate([peak_l, peak_r], 1)


def places(plan, tokens):
    parts = []
    for _, group, rows, _, _ in plan:
        shape = (up8(rows), tokens)
        row = lax.broadcasted_iota(jnp.int32, shape, 0)
        col = lax.broadcasted_iota(jnp.int32, shape, 1)
        part = col - row * group
        parts.append(part if rows % 8 == 0 else jnp.where(row < rows, part, -1))
    return parts


def exchange_kernel(plan, heads, scale, offs_hbm, q_hbm, k_hbm, v_hbm, *refs):
    number = len(plan)
    base_out, base_peak, base_total, hits_out = refs[:4]
    back = refs[4 : 4 + number]
    refs = refs[4 + number :]
    offs, q_ref, k_ref, v_ref = refs[:4]
    refs = refs[4:]
    stage = refs[:number]
    inbox = refs[number : 2 * number]
    outbox = refs[2 * number : 3 * number]
    in_sem, send_sem, recv_sem, ret_send, ret_recv, high_sem = refs[3 * number :]
    tokens, model = q_ref.shape
    size = model // heads
    pair = 2 * size
    pairs = heads // 2
    me = lax.axis_index("ctx")
    count = lax.axis_size("ctx")

    moves = [(offs_hbm, offs), (q_hbm, q_ref), (k_hbm, k_ref), (v_hbm, v_ref)]
    loads = [
        pltpu.make_async_copy(source, target, in_sem.at[i])
        for i, (source, target) in enumerate(moves)
    ]
    for load in loads:
        load.start()

    barrier = pltpu.get_barrier_semaphore()
    block = count // LINE
    line = lax.div(me, block)
    seat_in = me - line * block

    def tell(sem, other):
        pl.semaphore_signal(sem, inc=1, device_id=(other,), device_id_type=MESH)

    def greet(step, carry):
        tell(barrier, line * block + lax.rem(seat_in + step, block))
        return carry

    def greet_above(step, carry):
        tell(barrier, line * block + block + step)
        return carry

    with jax.named_scope("greet"):
        lax.fori_loop(1, block, greet, 0)
        lax.fori_loop(0, (LINE - 1 - line) * block, greet_above, 0)

    def hear(first, last):
        for at in range(LINE):
            for above in range(max(first, at + 1), last + 1):

                @pl.when(line == at)
                def _(above=above):
                    pl.semaphore_wait(high_sem.at[above], 1)

    low = halves((tokens, pair))
    spans = [up8(entry[2]) for entry in plan]
    starts = [sum(spans[:at]) for at in range(number)]
    picked = sum(spans)
    low_p = halves((picked, pair))
    where_p = places(plan, tokens)

    def meet():
        with jax.named_scope("barw"):
            pl.semaphore_wait(barrier, block - 1 + line * block)

        for at in range(1, LINE):
            for below in range(at):

                @pl.when(line == at)
                def _(at=at, below=below):
                    tell(high_sem.at[at], me - (at - below) * block)

    soon = line < LINE // 2

    @pl.when(jnp.logical_not(soon))
    def _():
        meet()

    with jax.named_scope("loadw"):
        for load in loads:
            load.wait()

    def pick(p, carry):
        cols = pl.ds(pl.multiple_of(p * pair, pair), pair)
        packed = jnp.concatenate([q_ref[:, cols], k_ref[:, cols], v_ref[:, cols]], 1)
        hits = []
        for side in range(2):
            for at, (height, *_) in enumerate(plan):
                hits.append(jnp.where(where_p[at] == offs[height, 2 * p + side], 1.0, 0.0))
        hit = jnp.concatenate(hits, 0).astype(jnp.bfloat16)
        hits_out[p] = hit
        both = jnp.dot(hit, packed, preferred_element_type=jnp.float32)
        for side in range(2):
            head = 2 * p + side
            got = both[side * picked : (side + 1) * picked]
            query, key, value = got[:, :pair], got[:, pair : 2 * pair], got[:, 2 * pair :]
            swapped = swap_halves(value)
            if side == 0:
                key = swap_halves(key)
            else:
                query = swap_halves(query)
                value, swapped = swapped, value
            left = jnp.where(low_p, query * scale, key)
            for at, (_, _, rows, *_) in enumerate(plan):
                kind = stage[at].dtype
                first = starts[at]
                last = first + rows
                if is_packed(rows):
                    middle = first + rows // 2
                    right = jnp.where(
                        low_p[: rows // 2], value[first:middle], swapped[middle:last]
                    )
                    stage[at][head] = jnp.concatenate([left[first:last], right], 0).astype(kind)
                else:
                    stage[at][head] = jnp.concatenate(
                        [left[first:last], value[first:last]], 1
                    ).astype(kind)
        return carry

    with jax.named_scope("pick"):
        lax.fori_loop(0, pairs, pick, 0, unroll=6)
    @pl.when(soon)
    def _():
        meet()

    seats, seat = [], 0
    for _, _, _, per, *_ in plan:
        seats.append(seat)
        seat += per

    def spot(at):
        _, group, _, per, owners = plan[at]
        mine = lax.rem(me, group)
        found = heads
        for head in range(0, heads, per):
            found = jnp.where(mine == owners[head], head, found)
        return mine, found

    spots = [spot(at) for at in range(number)]
    order = list(range(number))[::-1]

    def push(at, slots=None, only=None):
        _, group, _, per, *_ = plan[at]
        mine, _ = spots[at]
        for head in sorted(range(heads), key=lambda h: h % per):
            where = plan[at][4][head]
            slot = head % per
            if only is not None and head != only:
                continue
            if slots is not None and slot not in slots:
                continue
            target = inbox[at].at[slot, mine]
            arrived = recv_sem.at[seats[at] + slot]

            @pl.when(mine != where)
            def _(head=head, where=where, target=target, arrived=arrived):
                pltpu.make_async_remote_copy(
                    src_ref=stage[at].at[head],
                    dst_ref=target,
                    send_sem=send_sem.at[at],
                    recv_sem=arrived,
                    device_id=(me - mine + where,),
                    device_id_type=MESH,
                ).start()

            @pl.when(mine == where)
            def _(head=head, target=target, arrived=arrived):
                pltpu.make_async_copy(stage[at].at[head], target, arrived).start()

    ones = jnp.ones((16, tokens), jnp.bfloat16)
    row8 = lax.broadcasted_iota(jnp.int32, (8, tokens), 0)

    def base(p, carry):
        cols = pl.ds(pl.multiple_of(p * pair, pair), pair)
        query = q_ref[:, cols].astype(jnp.float32) * scale
        key = k_ref[:, cols]
        value_t = v_ref[:, cols].T
        for side in range(2):
            mask = low if side == 0 else jnp.logical_not(low)
            got, peak = attend(
                key,
                jnp.where(mask, query, 0.0).astype(jnp.bfloat16),
                jnp.concatenate([value_t[side * size : (side + 1) * size], ones], 0),
            )
            head = 2 * p + side
            base_out[head] = got[:size]
            base_peak[head] = jnp.where(row8 == number, peak, NEG)
            base_total[head] = jnp.where(row8 == number, got[size : size + 1], 1.0)
        return carry

    def bases(start, stop):
        start, stop = pairs * start // 6, pairs * stop // 6
        with jax.named_scope(f"base{start}"):
            lax.fori_loop(start, stop, base, 0, unroll=2)


    def returning(at, slot, head, there):
        _, _, rows, *_ = plan[at]
        mine, _ = spots[at]
        return pltpu.make_async_remote_copy(
            src_ref=outbox[at].at[slot, there],
            dst_ref=back[at].at[head, pl.ds(0, rows)],
            send_sem=ret_send.at[seats[at] + slot],
            recv_sem=ret_recv.at[at],
            device_id=(me - mine + there,),
            device_id_type=MESH,
        )

    row16 = lax.broadcasted_iota(jnp.int32, (16, tokens), 0)
    blank = jnp.zeros((pair - size - 16, tokens), jnp.bfloat16)

    def serve(at, slot):
        _, group, rows, per, *_ = plan[at]
        mine, first = spots[at]
        head = first + slot

        @pl.when(head < heads)
        def _():
            with jax.named_scope(f"arr{at}_{slot}"):
                pltpu.make_async_copy(
                    inbox[at].at[slot], inbox[at].at[slot], recv_sem.at[seats[at] + slot]
                ).wait()
            block = inbox[at][slot]
            if is_packed(rows):
                left = block[:, :rows].reshape(tokens, pair).astype(jnp.float32)
                right = block[:, rows:].reshape(tokens // 2, pair).astype(jnp.float32)
                split = (group, rows // 2, pair)
                right = jnp.concatenate(
                    [right.reshape(split), swap_halves(right).reshape(split)], 1
                ).reshape(tokens, pair)
            else:
                block = block.reshape(tokens, 2 * pair)
                left = block[:, :pair].astype(jnp.float32)
                right = block[:, pair:].astype(jnp.float32)
            value = jnp.where(low, right, 1.0).astype(jnp.bfloat16)
            query = jnp.where(low, left, 0.0).astype(jnp.bfloat16)
            key = swap_halves(left).astype(jnp.bfloat16)
            value_t = value.T[: size + 16]
            got, peak = attend(key, query, value_t)
            sums = got[size : size + 1]
            lse = peak + jnp.log(sums)
            high = lse.astype(jnp.bfloat16).astype(jnp.float32)
            rest = lse - high
            mid = rest.astype(jnp.bfloat16).astype(jnp.float32)
            parts = jnp.where(row16 == 0, high, 0.0)
            parts = jnp.where(row16 == 1, mid, parts)
            parts = jnp.where(row16 == 2, rest - mid, parts)
            result = jnp.concatenate(
                [
                    (got[:size] / sums).astype(jnp.bfloat16),
                    parts.astype(jnp.bfloat16),
                    blank,
                ],
                0,
            )
            outbox[at][slot] = (
                result.T.reshape(group, rows, pair).astype(outbox[at].dtype)
            )

            def give(there, carry):
                @pl.when(there != mine)
                def _():
                    returning(at, slot, head, there).start()

                return carry

            with jax.named_scope(f"give{at}_{slot}"):
                pltpu.make_async_copy(
                    outbox[at].at[slot, mine],
                    back[at].at[head, pl.ds(0, rows)],
                    ret_recv.at[at],
                ).start()
                lax.fori_loop(0, group, give, 0, unroll=group <= 32)

    last = line == LINE - 1
    soon_slots = range(1)
    rest_slots = range(1, plan[0][3])

    @pl.when(jnp.logical_not(last))
    def _():
        with jax.named_scope("push0"):
            push(0, soon_slots)

    @pl.when(soon)
    def _():
        bases(0, 2)

    far = [at for at in order if plan[at][1] >= 2 * heads]
    close = [at for at in order[:-1] if at not in far]

    @pl.when(soon)
    def _():
        hear(1, 1)
        for at in close:
            push(at)

    with jax.named_scope("hear"):
        hear(2, LINE - 2)
    with jax.named_scope("push1"):
        for head in range(heads):
            for at in far:
                push(at, only=head)

    @pl.when(jnp.logical_not(soon))
    def _():
        hear(LINE - 1, LINE - 1)
        for at in close:
            push(at)

    @pl.when(last)
    def _():
        with jax.named_scope("push0b"):
            push(0)

    @pl.when(jnp.logical_not(last))
    def _():
        with jax.named_scope("push0c"):
            push(0, rest_slots)

    with jax.named_scope("late"):
        pl.when(soon)(lambda: hear(LINE - 1, LINE - 1))

    @pl.when(jnp.logical_not(soon))
    def _():
        bases(0, 2)

    wide = [(at, slot) for at in order[:-1] for slot in range(plan[at][3])]
    tall = [(0, slot) for slot in range(plan[0][3])]

    def serve_all(jobs):
        for at, slot in jobs:
            serve(at, slot)

    @pl.when(last)
    def _():
        serve_all(wide + tall)

    @pl.when(soon)
    def _():
        serve_all(tall[:1] + wide[-1:] + wide[:-1] + tall[1:])

    @pl.when(jnp.logical_not(jnp.logical_or(soon, last)))
    def _():
        serve_all(tall[:1] + wide + tall[1:])

    bases(2, 6)
    for at in order:
        _, group, rows, per, *_ = plan[at]
        _, first = spots[at]
        owned = jnp.clip(heads - first, 0, per)
        with jax.named_scope(f"coll{at}"):
            for many in range(per + 1):

                @pl.when(owned == many)
                def _(at=at, many=many):
                    sent = stage[at].at[pl.ds(0, heads - many)]
                    pltpu.make_async_copy(sent, sent, send_sem.at[at]).wait()

            landed = back[at].at[:, pl.ds(0, rows)]
            pltpu.make_async_copy(landed, landed, ret_recv.at[at]).wait()

    for at in order:
        _, group, _, per, *_ = plan[at]
        _, first = spots[at]
        for slot in range(per):

            @pl.when(first + slot < heads)
            def _(at=at, group=group, slot=slot):
                gone = outbox[at].at[slot, pl.ds(0, group - 1)]
                pltpu.make_async_copy(gone, gone, ret_send.at[seats[at] + slot]).wait()


def merge_kernel(plan, heads, base_out, base_peak, base_total, hits, *refs):
    number = len(plan)
    back = refs[:number]
    out_hbm, out_vmem, sem = refs[number:]
    tokens, model = out_vmem.shape
    size = model // heads
    pair = 2 * size
    pairs = heads // 2
    spans = [up8(entry[2]) for entry in plan]
    picked = sum(spans)
    row8 = lax.broadcasted_iota(jnp.int32, (8, picked), 0)
    col8 = lax.broadcasted_iota(jnp.int32, (8, picked), 1)
    level = jnp.zeros((8, picked), jnp.int32)
    for at in range(1, number):
        level = jnp.where(col8 >= sum(spans[:at]), at, level)
    mine = row8 == level
    flag = jnp.where(mine, 1.0, 0.0)

    def leave(p):
        cols = pl.ds(p * pair, pair)
        return pltpu.make_async_copy(out_vmem.at[:, cols], out_hbm.at[:, cols], sem.at[p])

    sents, sums, shares = {}, {}, {}
    for p in range(pairs):
        for side in range(2):
            head = 2 * p + side
            blocks = []
            for at, (_, _, rows, *_) in enumerate(plan):
                block = back[at][head].astype(jnp.float32)
                if rows % 8:
                    kept = lax.broadcasted_iota(jnp.int32, block.shape, 0) < rows
                    block = jnp.where(kept, block, 0.0)
                blocks.append(block)
            sent_t = jnp.concatenate(blocks, 0).astype(jnp.bfloat16).T
            hit = hits[p, side * picked : (side + 1) * picked]
            tails = sent_t[size : size + 16].astype(jnp.float32)
            parts = [jnp.where(mine, tails[i : i + 1], 0.0) for i in range(3)]
            parts = jnp.concatenate(parts + [flag], 0).astype(jnp.bfloat16)
            lses = jnp.dot(parts, hit, preferred_element_type=jnp.float32)
            sents[head], sums[head] = sent_t, lses
    for p in range(pairs):
        for side in range(2):
            head = 2 * p + side
            lses = sums[head]
            lse = lses[:8] + lses[8:16] + lses[16:24]
            lse = jnp.where(lses[24:] > 0.5, lse, base_peak[head])
            best = jnp.max(lse, axis=0, keepdims=True)
            share = jnp.exp(lse - best)
            bottom = jnp.sum(share * base_total[head], axis=0, keepdims=True)
            share = share / bottom
            shares[head] = share
    for p in range(pairs):
        merged = []
        for side in range(2):
            head = 2 * p + side
            sent_t, share = sents[head], shares[head]
            hit = hits[p, side * picked : (side + 1) * picked]
            spread = jnp.concatenate(
                [
                    jnp.broadcast_to(share[at : at + 1], (spans[at], tokens))
                    for at in range(number)
                ],
                0,
            )
            moved = jnp.dot(
                sent_t[:size],
                hit * spread.astype(jnp.bfloat16),
                preferred_element_type=jnp.float32,
            )
            merged.append(moved + share[number : number + 1] * base_out[head])
        both = jnp.concatenate(merged, 0).astype(jnp.bfloat16)
        out_vmem[:, pl.ds(p * pair, pair)] = both.T
        leave(p).start()
    for p in range(pairs):
        leave(p).wait()


def exchange_body(queries, keys, values, offsets):
    tokens, model = queries.shape
    levels, heads = offsets.shape
    count = lax.axis_size("ctx")
    plan = plan_of(levels, count, tokens, heads)
    size = model // heads
    pair = 2 * size
    number = len(plan)
    seats = sum(entry[3] for entry in plan)
    picked = sum(up8(entry[2]) for entry in plan)

    def block(rows):
        return (rows + rows // 2, pair) if is_packed(rows) else (rows, 2 * pair)

    scratch = [pltpu.SMEM((levels, heads), jnp.int32)]
    scratch += [pltpu.VMEM((tokens, model), jnp.bfloat16)] * 3
    for _, group, rows, per, *_ in plan:
        scratch.append(pltpu.VMEM((heads, *block(rows)), kind_of(rows)))
    for _, group, rows, per, *_ in plan:
        scratch.append(pltpu.VMEM((per, group, *block(rows)), kind_of(rows)))
    for _, group, rows, per, *_ in plan:
        scratch.append(pltpu.VMEM((per, group, rows, pair), kind_of(rows)))
    scratch += [
        pltpu.SemaphoreType.DMA((4,)),
        pltpu.SemaphoreType.DMA((number,)),
        pltpu.SemaphoreType.DMA((seats,)),
        pltpu.SemaphoreType.DMA((seats,)),
        pltpu.SemaphoreType.DMA((number,)),
        pltpu.SemaphoreType.REGULAR((LINE,)),
    ]
    outs = [
        pltpu.VMEM((heads, size, tokens), jnp.float32),
        pltpu.VMEM((heads, 8, tokens), jnp.float32),
        pltpu.VMEM((heads, 8, tokens), jnp.float32),
        pltpu.VMEM((heads // 2, 2 * picked, tokens), jnp.bfloat16),
    ]
    for _, _, rows, *_ in plan:
        outs.append(pltpu.VMEM((heads, up8(rows), pair), kind_of(rows)))
    scale = size**-0.5
    vmem = pl.BlockSpec(memory_space=pltpu.VMEM)
    far = pl.BlockSpec(memory_space=pl.ANY)
    parts = pl.pallas_call(
        functools.partial(exchange_kernel, plan, heads, scale),
        out_shape=outs,
        in_specs=[far, far, far, far],
        out_specs=[vmem] * len(outs),
        scratch_shapes=scratch,
        compiler_params=pltpu.CompilerParams(collective_id=0, has_side_effects=True),
    )(offsets, queries, keys, values)
    return pl.pallas_call(
        functools.partial(merge_kernel, plan, heads),
        out_shape=jax.ShapeDtypeStruct((tokens, model), jnp.bfloat16),
        in_specs=[vmem] * len(outs),
        out_specs=far,
        scratch_shapes=[
            pltpu.VMEM((tokens, model), jnp.bfloat16),
            pltpu.SemaphoreType.DMA((heads // 2,)),
        ],
        compiler_params=pltpu.CompilerParams(vmem_limit_bytes=16 * 1024 * 1024),
    )(*parts)


def solution(mesh):
    in_specs = (P("ctx", None), P("ctx", None), P("ctx", None), P())
    out_specs = P("ctx", None)
    return jax.shard_map(
        exchange_body, mesh=mesh, in_specs=in_specs, out_specs=out_specs, check_vma=False
    )
```
